32 devices in a mesh: rows: 16 (over z, y, x), cols: 2 (over core).
Axes of the slice: x: 2, y: 2, z: 4, core: 2. Of those that a mesh axis runs over, the one named last changes fastest.
Arguments:
- green: float32 [2, 4096, 4096], P('cols', 'rows'), may hold values from -1 to 1, as said below
- sites: int32 [16], replicated, may hold values from 0 to 4095, as said below
- fields: int32 [4096], replicated, may hold values from 0 to 1
- accept: int32 [16], replicated, may hold values 0 or 1
Outputs:
- green_new: float32 [2, 4096, 4096], P('cols', 'rows')
- log_weight: float32 [], replicated
The draws below stay inside these ranges and needn't reach their ends.
Inputs may be any that keep to these rules, and one draw needn't show every extreme that they name: The 16 proposed sites are distinct. `green`: each spin's matrix has its diagonal within 0.1 to 0.9 and off-diagonal entries of size about 1 / sqrt(4096).
All inputs are finite; a program needn't handle non-finite values.
Results may differ from the reference program's by a relative error of at most 0.0003.
Values sent between devices are 32-bit elements; how exact they have to be, the bound alone decides.
A program may use at most 64 MiB of HBM per device.

```python
import math
import jax
import jax.numpy as jnp
from jax import lax

N = 4096
K = 16


def draw_green(key, part):
    first, second = jax.random.split(jax.random.fold_in(key, 11))
    diag = jax.random.uniform(first, (2, N), jnp.float32, 0.2, 0.8)
    off = jax.random.normal(second, (2, N, N), jnp.float32) * (0.7 / math.sqrt(N))
    unit = jnp.eye(N, dtype=jnp.float32)
    return off * (1.0 - unit) + unit * diag[:, :, None]


def draw_sites(key, part):
    order = jax.random.permutation(jax.random.fold_in(key, 23), N)
    return order[:K].astype(jnp.int32)


def place_ends(result, own_key, smallest, high):
    longest = result.shape.index(max(result.shape))
    spots = []
    for shift in (0, 1):
        where = [jax.random.randint(jax.random.fold_in(own_key, axis), (), 0, length) for axis, length in enumerate(result.shape)]
        where[longest] = (where[longest] + shift) % result.shape[longest]
        spots.append(tuple(where))
    return result.at[spots[0]].set(smallest).at[spots[1]].set(high)


def setup_inputs(seed: int = 0) -> dict:
    key_of = jax.random.split(jax.random.key(seed), 5)
    green = draw_green(jax.random.fold_in(key_of[4], 71), 0)
    sites = draw_sites(jax.random.fold_in(key_of[4], 71), 0)
    fields = place_ends(jax.random.randint(key_of[2], (N,), 0, 2), jax.random.fold_in(key_of[2], 1), 0, 1).astype(jnp.int32)
    accept = place_ends((jax.random.randint(key_of[3], (K,), 0, 2) < 1).astype(jnp.int32), jax.random.fold_in(key_of[3], 1), 0, 1)
    return dict(green=green, sites=sites, fields=fields, accept=accept)


FLOOR = 0.25
COUPLING = 0.5


def sweep(green, sigma, sites, fields, accept):
    width = green.shape[0]
    steps = sites.shape[0]
    spins = 1.0 - 2.0 * jnp.take(fields, sites).astype(green.dtype)
    deltas = jnp.exp(-2.0 * COUPLING * sigma * spins) - 1.0
    flags = accept.astype(green.dtype)
    positions = lax.broadcasted_iota(jnp.int32, (1, width), 1)

    def step(k, state):
        u_all, v_all, weight = state
        site = sites[k]
        row = lax.dynamic_slice_in_dim(green, site, 1, 0) - jnp.dot(
            lax.dynamic_slice_in_dim(u_all, site, 1, 0), v_all.T, precision=lax.Precision.HIGHEST)
        v_site = lax.dynamic_slice_in_dim(v_all, site, 1, 0)
        column = lax.dynamic_slice_in_dim(green, site, 1, 1)[:, 0] - jnp.dot(
            u_all, v_site[0], precision=lax.Precision.HIGHEST)
        diag = lax.dynamic_slice_in_dim(row[0], site, 1)[0]
        ratio = jnp.maximum(1.0 + deltas[k] * (1.0 - diag), FLOOR)
        coef = flags[k] * deltas[k] / ratio
        u_all = lax.dynamic_update_slice_in_dim(u_all, (coef * column)[:, None], k, 1)
        fresh = (positions == site).astype(green.dtype) - row
        v_all = lax.dynamic_update_slice_in_dim(v_all, fresh.T, k, 1)
        weight = weight + flags[k] * jnp.log(ratio)
        return (u_all, v_all, weight)

    start = (jnp.zeros((width, steps), green.dtype), jnp.zeros((width, steps), green.dtype), jnp.zeros((), green.dtype))
    u_all, v_all, weight = lax.fori_loop(0, steps, step, start)
    return green - jnp.dot(u_all, v_all.T, precision=lax.Precision.HIGHEST), weight


def reference(green, sites, fields, accept):
    up_new, up_weight = sweep(green[0], 1.0, sites, fields, accept)
    down_new, down_weight = sweep(green[1], -1.0, sites, fields, accept)
    return jnp.stack([up_new, down_new]), up_weight + down_weight
```

```python
import functools

import jax
import jax.numpy as jnp
import numpy as np
from jax import lax
from jax.experimental import pallas as pl
from jax.experimental.pallas import tpu as pltpu
from jax.sharding import PartitionSpec as P

FLOOR = 0.25
COUPLING = 0.5
LANES = 128
MESH = pl.DeviceIdType.MESH


def pick_kernel(n, steps, rows_dev, width, cc, rg,
                sites_ref, fields_ref, accept_ref, local,
                picked, blk, spread_ref, site_ref, delta_ref, flag_ref):
    spin = lax.axis_index("cols")
    prow = steps // rg
    pcol = width // cc
    per = LANES // steps
    brow = steps // per
    first = lax.axis_index("rows") * rows_dev
    site = [sites_ref[k] for k in range(steps)]

    for k in range(steps):
        rel = site[k] - first
        inside = jnp.logical_and(rel >= 0, rel < rows_dev)
        row = local[pl.ds(jnp.clip(rel, 0, rows_dev - 1), 1), :]
        row = jnp.where(inside, row, 0.0)
        for c in range(cc):
            picked[(k // prow) * cc + c, k % prow:k % prow + 1, :] = row[:, c * pcol:(c + 1) * pcol]

    lane = lax.broadcasted_iota(jnp.int32, (steps, LANES), 1)
    sub = lax.broadcasted_iota(jnp.int32, (steps, LANES), 0)
    spread = jnp.zeros((rows_dev, LANES), jnp.float32)
    lane_c = lax.broadcasted_iota(jnp.int32, (rows_dev, LANES), 1)
    for j in range(steps):
        tile = pl.multiple_of((site[j] // LANES) * LANES, LANES)
        strip = local[:, pl.ds(tile, LANES)]
        value = jnp.sum(jnp.where(lane_c == site[j] - tile, strip, 0.0), axis=1, keepdims=True)
        spread = jnp.where(lane_c == j, value, spread)
    spread_ref[...] = spread

    block = jnp.zeros((steps, LANES), jnp.float32)
    sites_all = jnp.zeros((steps, LANES), jnp.int32)
    deltas = jnp.zeros((steps, LANES), jnp.float32)
    flags = jnp.zeros((steps, LANES), jnp.float32)
    same = np.float32(np.exp(np.float32(-2.0 * COUPLING))) - np.float32(1.0)
    differ = np.float32(np.exp(np.float32(2.0 * COUPLING))) - np.float32(1.0)
    for k in range(steps):
        rel = site[k] - first
        inside = jnp.logical_and(rel >= 0, rel < rows_dev)
        line = spread_ref[pl.ds(jnp.clip(rel, 0, rows_dev - 1), 1), :]
        line = jnp.where(inside, line, 0.0)
        block = jnp.where(sub == k, jnp.broadcast_to(line, block.shape), block)
        sites_all = jnp.where(sub == k, site[k], sites_all)
        delta = jnp.where(fields_ref[site[k]] == spin, same, differ)
        deltas = jnp.where(sub == k, delta, deltas)
        flags = jnp.where(sub == k, accept_ref[k].astype(jnp.float32), flags)
    site_ref[...] = sites_all
    delta_ref[...] = deltas
    flag_ref[...] = flags

    packed = []
    for q in range(brow):
        line = block[q * per:(q + 1) * per, :]
        sub_q = lax.broadcasted_iota(jnp.int32, (per, LANES), 0)
        acc = jnp.zeros((per, LANES), jnp.float32)
        for i in range(per):
            turned = line if i == 0 else pltpu.roll(line, i * steps, 1)
            acc = jnp.where(sub_q == i, turned, acc)
        packed.append(jnp.sum(acc, axis=0, keepdims=True))
    blk[...] = jnp.concatenate(packed, axis=0)


def exchange_kernel(n, steps, rows_dev, width, cc, rg,
                    picked, blk, spread_ref, site_ref, delta_ref, flag_ref,
                    ust_ref, vst_ref, total_ref,
                    landed, mine, raw, blks, wgt, wgt_in,
                    s1, r1, s2, r2, sb, rb, sw, rw):
    me = lax.axis_index("rows")
    other = 1 - lax.axis_index("cols")
    pcol = width // cc
    per = LANES // steps
    barrier = pltpu.get_barrier_semaphore()

    def greet(j, _):
        pl.semaphore_signal(barrier, inc=1, device_id={"rows": lax.rem(me + j, n)}, device_id_type=MESH)
        return _

    lax.fori_loop(1, n, greet, 0)
    pl.semaphore_signal(barrier, inc=1, device_id={"cols": other}, device_id_type=MESH)
    lane = lax.broadcasted_iota(jnp.int32, (steps, LANES), 1)
    sub = lax.broadcasted_iota(jnp.int32, (steps, LANES), 0)
    pl.semaphore_wait(barrier, n)

    def order(i):
        return 1 + lax.rem(i + n // 2 - 1, n - 1)

    def block_copy(j):
        to = lax.rem(me + j, n)
        return pltpu.make_async_remote_copy(
            src_ref=blk, dst_ref=blks.at[j], send_sem=sb.at[j], recv_sem=rb.at[j],
            device_id={"rows": to}, device_id_type=MESH)

    def first_copy(j):
        to = lax.rem(me + j, n)
        return pltpu.make_async_remote_copy(
            src_ref=picked.at[to], dst_ref=landed.at[j], send_sem=s1.at[j], recv_sem=r1.at[j],
            device_id={"rows": to}, device_id_type=MESH)

    def second_copy(j):
        to = lax.rem(me + j, n)
        return pltpu.make_async_remote_copy(
            src_ref=mine, dst_ref=raw.at[me], send_sem=s2.at[j], recv_sem=r2.at[j],
            device_id={"rows": to}, device_id_type=MESH)

    def each(fn):
        def body(i, _):
            fn(order(i))
            return _
        lax.fori_loop(0, n - 1, body, 0)

    each(lambda j: block_copy(j).start())
    each(lambda j: first_copy(j).start())

    each(lambda j: first_copy(j).wait_recv())
    chunk = picked[me]
    for j in range(1, n):
        chunk = chunk + landed[j]
    mine[...] = chunk
    raw[me] = chunk
    each(lambda j: second_copy(j).start())

    each(lambda j: block_copy(j).wait_recv())
    packed = blk[...]
    for j in range(1, n):
        packed = packed + blks[j]
    block = jnp.zeros((steps, LANES), jnp.float32)
    for k in range(steps):
        line = jnp.broadcast_to(packed[k // per:k // per + 1, :], (8, LANES))
        back = (LANES - (k % per) * steps) % LANES
        if back:
            line = pltpu.roll(line, back, 1)
        block = jnp.where(sub == k, jnp.broadcast_to(line[0:1, :], (steps, LANES)), block)
    one = jnp.float32(1.0)
    block = jnp.where(lane < steps, block, jnp.where(lane == sub + steps, one, 0.0))
    under = jnp.where(lane == sub, one, 0.0)
    z = jnp.concatenate([block, under], axis=0)
    lane_1 = lax.broadcasted_iota(jnp.int32, (1, LANES), 1)
    ratios = jnp.ones((1, LANES), jnp.float32)
    flags = jnp.zeros((1, LANES), jnp.float32)
    for k in range(steps):
        flag = flag_ref[k:k + 1, :]
        delta = delta_ref[k:k + 1, :]
        row = z[k:k + 1, :]
        column = jnp.broadcast_to(z[:, k:k + 1], z.shape)
        diag = column[k:k + 1, :]
        ratio = jnp.maximum(1.0 + delta * (1.0 - diag), FLOOR)
        coef = (flag * delta) / ratio
        fresh = jnp.where(lane_1 == k, one, 0.0) - row
        z = z - column * (coef * fresh)
        ratios = jnp.where(lane_1 == k, ratio, ratios)
        flags = jnp.where(lane_1 == k, flag, flags)
    weight = jnp.sum(flags * jnp.log(ratios), axis=1, keepdims=True)
    wgt[...] = jnp.broadcast_to(weight, (8, LANES))
    swap = pltpu.make_async_remote_copy(
        src_ref=wgt, dst_ref=wgt_in, send_sem=sw, recv_sem=rw,
        device_id={"cols": other}, device_id_type=MESH)
    swap.start()

    w = pltpu.roll(z[steps:2 * steps, :], LANES - steps, 1)
    w = jnp.where(lane < steps, w, 0.0)
    w = w + pltpu.roll(w, steps, 1) + pltpu.roll(w, 2 * steps, 1)
    w = jnp.concatenate([w, jnp.zeros((LANES - steps, LANES), jnp.float32)], axis=0)
    u = jnp.dot(spread_ref[...], w, precision=lax.Precision.HIGHEST, preferred_element_type=jnp.float32)
    lane_c = lax.broadcasted_iota(jnp.int32, (rows_dev, LANES), 1)
    high = u.astype(jnp.bfloat16).astype(jnp.float32)
    ust_ref[...] = jnp.where(lane_c < 2 * steps, high, u - high).astype(jnp.bfloat16)

    lane_p = lax.broadcasted_iota(jnp.int32, (steps, pcol), 1)
    owner = jnp.broadcast_to(site_ref[:, 0:1], (steps, pcol)) - lane_p

    each(lambda j: second_copy(j).wait_recv())
    for c in range(cc):
        parts = [raw[g * cc + c] for g in range(rg)]
        rows = parts[0] if rg == 1 else jnp.concatenate(parts, axis=0)
        v = jnp.where(owner == c * pcol, one, 0.0) - rows
        vh = v.astype(jnp.bfloat16)
        vl = (v - vh.astype(jnp.float32)).astype(jnp.bfloat16)
        vst_ref[:, c * pcol:(c + 1) * pcol] = jnp.concatenate([vh, vl, vh], axis=0)

    swap.wait()
    total_ref[0, 0] = jnp.max(wgt[0:1, :] + wgt_in[0:1, :])
    each(lambda j: block_copy(j).wait_send())
    each(lambda j: first_copy(j).wait_send())
    each(lambda j: second_copy(j).wait_send())


def apply_kernel(k3, tile, ust_ref, vst_ref, total_ref, local, out_ref, sum_ref):
    cols = pl.ds(pl.multiple_of(pl.program_id(0) * tile, tile), tile)
    out_ref[...] = local[:, cols] - jnp.dot(
        ust_ref[:, :k3], vst_ref[...], preferred_element_type=jnp.float32)
    sum_ref[0, 0] = total_ref[0, 0]


def on_device(n, green, sites, fields, accept):
    local = green[0]
    rows_dev, width = local.shape
    steps = sites.shape[0]
    cc = min(n, width // LANES)
    rg = n // cc
    brow = steps // (LANES // steps)
    prow, pcol = steps // rg, width // cc
    f32, i32, bf16 = jnp.float32, jnp.int32, jnp.bfloat16
    vmem = pl.BlockSpec(memory_space=pltpu.VMEM)
    smem = pl.BlockSpec(memory_space=pltpu.SMEM)
    dma = pltpu.SemaphoreType.DMA
    shape = jax.ShapeDtypeStruct
    limit = 16 * 1024 * 1024
    sizes = (n, steps, rows_dev, width, cc, rg)
    parts = pl.pallas_call(
        functools.partial(pick_kernel, *sizes),
        out_shape=(
            shape((n, prow, pcol), f32), shape((brow, LANES), f32), shape((rows_dev, LANES), f32),
            shape((steps, LANES), i32), shape((steps, LANES), f32), shape((steps, LANES), f32),
        ),
        in_specs=[smem, smem, smem, vmem],
        out_specs=(vmem,) * 6,
        compiler_params=pltpu.CompilerParams(vmem_limit_bytes=limit),
        cost_estimate=pl.CostEstimate(flops=10 ** 6, bytes_accessed=4 * rows_dev * width, transcendentals=0),
        name="pick",
    )(sites, fields, accept, local)

    ust, vst, total = pl.pallas_call(
        functools.partial(exchange_kernel, *sizes),
        out_shape=(shape((rows_dev, LANES), bf16), shape((3 * steps, width), bf16), shape((1, 1), f32)),
        in_specs=[vmem] * 6,
        out_specs=(vmem, vmem, smem),
        scratch_shapes=[
            pltpu.VMEM((n, prow, pcol), f32),
            pltpu.VMEM((prow, pcol), f32),
            pltpu.VMEM((n, prow, pcol), f32),
            pltpu.VMEM((n, brow, LANES), f32),
            pltpu.VMEM((8, LANES), f32),
            pltpu.VMEM((8, LANES), f32),
            dma((n,)), dma((n,)), dma((n,)), dma((n,)), dma((n,)), dma((n,)), dma, dma,
        ],
        compiler_params=pltpu.CompilerParams(
            collective_id=0, has_side_effects=True, vmem_limit_bytes=limit),
        cost_estimate=pl.CostEstimate(flops=10 ** 9, bytes_accessed=64 * 2 ** 20, transcendentals=0),
        name="exchange",
    )(*parts)

    tile = min(512, width)
    updated, summed = pl.pallas_call(
        functools.partial(apply_kernel, 3 * steps, tile),
        grid=(width // tile,),
        out_shape=(shape((rows_dev, width), f32), shape((1, 1), f32)),
        in_specs=[vmem, pl.BlockSpec((3 * steps, tile), lambda i: (0, i)), smem, vmem],
        out_specs=(pl.BlockSpec((rows_dev, tile), lambda i: (0, i)), smem),
        compiler_params=pltpu.CompilerParams(vmem_limit_bytes=limit),
        cost_estimate=pl.CostEstimate(
            flops=2 * rows_dev * width * 3 * steps, bytes_accessed=8 * rows_dev * width, transcendentals=0),
        name="apply",
    )(ust, vst, total, local)
    return updated[None], summed.reshape(())


def solution(mesh):
    in_specs = (P("cols", "rows", None), P(), P(), P())
    out_specs = (P("cols", "rows", None), P())
    return jax.shard_map(
        functools.partial(on_device, mesh.shape["rows"]),
        mesh=mesh, in_specs=in_specs, out_specs=out_specs, check_vma=False,
    )
```

```python
import functools

import jax
import jax.numpy as jnp
import numpy as np
from jax import lax
from jax.experimental import pallas as pl
from jax.experimental.pallas import tpu as pltpu
from jax.sharding import PartitionSpec as P

FLOOR = 0.25
COUPLING = 0.5
LANES = 128
MESH = pl.DeviceIdType.MESH


def exchange_kernel(n, steps, rows_dev, width, cc, rg,
                    sites_hbm, fields_hbm, accept_hbm, green_hbm,
                    ust_ref, vst_ref, total_ref,
                    sites_ref, fields_ref, accept_ref, local, picked, spread_ref,
                    landed, mine, raw, blk, blks, wgt, wgt_in,
                    ls, s1, r1, s2, r2, sb, rb, sw, rw):
    me = lax.axis_index("rows")
    spin = lax.axis_index("cols")
    other = 1 - spin
    prow = steps // rg
    pcol = width // cc
    per = LANES // steps
    brow = steps // per

    loads = [
        pltpu.make_async_copy(sites_hbm, sites_ref, ls.at[0]),
        pltpu.make_async_copy(accept_hbm, accept_ref, ls.at[1]),
        pltpu.make_async_copy(fields_hbm, fields_ref, ls.at[2]),
        pltpu.make_async_copy(green_hbm, local, ls.at[3]),
    ]
    for load in loads:
        load.start()

    barrier = pltpu.get_barrier_semaphore()

    def greet(j, _):
        pl.semaphore_signal(barrier, inc=1, device_id={"rows": lax.rem(me + j, n)}, device_id_type=MESH)
        return _

    lax.fori_loop(1, n, greet, 0)
    pl.semaphore_signal(barrier, inc=1, device_id={"cols": other}, device_id_type=MESH)

    first = me * rows_dev
    for load in loads:
        load.wait()
    site = [sites_ref[k] for k in range(steps)]
    lane = lax.broadcasted_iota(jnp.int32, (steps, LANES), 1)
    sub = lax.broadcasted_iota(jnp.int32, (steps, LANES), 0)
    lane_1 = lax.broadcasted_iota(jnp.int32, (1, LANES), 1)

    span = min(2 * LANES, width)
    site_sub = jnp.zeros((steps, rows_dev), jnp.int32)
    row_at = lax.broadcasted_iota(jnp.int32, (steps, rows_dev), 0)
    for k in range(steps):
        site_sub = jnp.where(row_at == k, site[k], site_sub)
    mark = lax.broadcasted_iota(jnp.int32, (steps, rows_dev), 1) + first
    chosen = jnp.where(site_sub == mark, 1.0, 0.0).astype(jnp.bfloat16)

    def split(x):
        h = x.astype(jnp.bfloat16)
        rest = x - h.astype(jnp.float32)
        m = rest.astype(jnp.bfloat16)
        return h, m, (rest - m.astype(jnp.float32)).astype(jnp.bfloat16)

    def mul(x, y):
        return jnp.dot(x, y, preferred_element_type=jnp.float32)

    for q in range(width // span):
        h, m, l = split(local[:, q * span:(q + 1) * span])
        got = mul(chosen, h) + mul(chosen, m) + mul(chosen, l)
        for t in range(span // LANES):
            p, o = divmod(q * span + t * LANES, pcol)
            for g in range(rg):
                picked[g * cc + p, :, o:o + LANES] = got[g * prow:(g + 1) * prow, t * LANES:(t + 1) * LANES]

    pl.semaphore_wait(barrier, n)

    def order(i):
        return 1 + lax.rem(i + n // 2 - 1, n - 1)

    def block_copy(j):
        to = lax.rem(me + j, n)
        return pltpu.make_async_remote_copy(
            src_ref=blk, dst_ref=blks.at[j], send_sem=sb.at[j], recv_sem=rb.at[j],
            device_id={"rows": to}, device_id_type=MESH)

    def first_copy(j):
        to = lax.rem(me + j, n)
        return pltpu.make_async_remote_copy(
            src_ref=picked.at[to], dst_ref=landed.at[j], send_sem=s1.at[j], recv_sem=r1.at[j],
            device_id={"rows": to}, device_id_type=MESH)

    def second_copy(j):
        to = lax.rem(me + j, n)
        return pltpu.make_async_remote_copy(
            src_ref=mine, dst_ref=raw.at[me], send_sem=s2.at[j], recv_sem=r2.at[j],
            device_id={"rows": to}, device_id_type=MESH)

    def each(fn):
        def body(i, _):
            fn(order(i))
            return _
        lax.fori_loop(0, n - 1, body, 0)

    each(lambda j: first_copy(j).start())

    site_lane = jnp.full((span, LANES), -1, jnp.int32)
    lane_s = lax.broadcasted_iota(jnp.int32, (span, LANES), 1)
    for k in range(steps):
        site_lane = jnp.where(lane_s == k, site[k], site_lane)
    site_lane = site_lane - lax.broadcasted_iota(jnp.int32, (span, LANES), 0)
    block = jnp.zeros((steps, LANES), jnp.float32)
    for q in range(width // span):
        wanted = jnp.where(site_lane == q * span, 1.0, 0.0).astype(jnp.bfloat16)
        pieces = []
        for t in range(span // LANES):
            p, o = divmod(q * span + t * LANES, pcol)
            parts = [picked[g * cc + p, :, o:o + LANES] for g in range(rg)]
            pieces.append(parts[0] if rg == 1 else jnp.concatenate(parts, axis=0))
        h, m, l = split(jnp.concatenate(pieces, axis=1))
        block = block + (mul(h, wanted) + mul(m, wanted) + mul(l, wanted))
    packed = []
    for q in range(brow):
        line = block[q * per:(q + 1) * per, :]
        sub_q = lax.broadcasted_iota(jnp.int32, (per, LANES), 0)
        acc = jnp.zeros((per, LANES), jnp.float32)
        for i in range(per):
            turned = line if i == 0 else pltpu.roll(line, i * steps, 1)
            acc = jnp.where(sub_q == i, turned, acc)
        packed.append(jnp.sum(acc, axis=0, keepdims=True))
    blk[...] = jnp.concatenate(packed, axis=0)
    each(lambda j: block_copy(j).start())

    spread = jnp.zeros((rows_dev, LANES), jnp.float32)
    lane_c = lax.broadcasted_iota(jnp.int32, (rows_dev, LANES), 1)
    for q in range(width // span):
        wanted = jnp.where(site_lane == q * span, 1.0, 0.0).astype(jnp.bfloat16)
        h, m, l = split(local[:, q * span:(q + 1) * span])
        spread = spread + (mul(h, wanted) + mul(m, wanted) + mul(l, wanted))
    spread_ref[...] = spread

    each(lambda j: first_copy(j).wait_recv())
    chunk = picked[me]
    for j in range(1, n):
        chunk = chunk + landed[j]
    mine[...] = chunk
    raw[me] = chunk
    each(lambda j: second_copy(j).start())

    each(lambda j: block_copy(j).wait_recv())
    packed = blk[...]
    for j in range(1, n):
        packed = packed + blks[j]
    block = jnp.zeros((steps, LANES), jnp.float32)
    for k in range(steps):
        line = jnp.broadcast_to(packed[k // per:k // per + 1, :], (8, LANES))
        back = (LANES - (k % per) * steps) % LANES
        if back:
            line = pltpu.roll(line, back, 1)
        block = jnp.where(sub == k, jnp.broadcast_to(line[0:1, :], (steps, LANES)), block)
    one = jnp.float32(1.0)
    block = jnp.where(lane < steps, block, jnp.where(lane == sub + steps, one, 0.0))
    under = jnp.where(lane == sub, one, 0.0)
    z = jnp.concatenate([block, under], axis=0)
    same = np.float32(np.exp(np.float32(-2.0 * COUPLING))) - np.float32(1.0)
    differ = np.float32(np.exp(np.float32(2.0 * COUPLING))) - np.float32(1.0)
    fields = fields_ref[...]
    place = (lax.broadcasted_iota(jnp.int32, fields.shape, 0) * LANES
             + lax.broadcasted_iota(jnp.int32, fields.shape, 1))
    deltas = []
    for k in range(steps):
        found = jnp.where(place == site[k], fields.astype(jnp.float32), 0.0)
        found = jnp.sum(jnp.sum(found, axis=0, keepdims=True), axis=1, keepdims=True)
        found = jnp.broadcast_to(found, (1, LANES)) * jnp.ones((1, LANES), jnp.float32)
        kind = jnp.where(spin + 0 * lane_1 == 0, found, 1.0 - found)
        deltas.append(same + kind * (differ - same))
    ratios = jnp.ones((1, LANES), jnp.float32)
    flags = jnp.zeros((1, LANES), jnp.float32)
    for k in range(steps):
        flag = accept_ref[k].astype(jnp.float32)
        delta = deltas[k]
        row = z[k:k + 1, :]
        column = jnp.broadcast_to(z[:, k:k + 1], z.shape)
        diag = column[k:k + 1, :]
        ratio = jnp.maximum(1.0 + delta * (1.0 - diag), FLOOR)
        coef = (flag * delta) / ratio
        fresh = jnp.where(lane_1 == k, one, 0.0) - row
        z = z - column * (coef * fresh)
        ratios = jnp.where(lane_1 == k, ratio, ratios)
        flags = jnp.where(lane_1 == k, flag, flags)
    weight = jnp.sum(flags * jnp.log(ratios), axis=1, keepdims=True)
    wgt[...] = jnp.broadcast_to(weight, (8, LANES))
    swap = pltpu.make_async_remote_copy(
        src_ref=wgt, dst_ref=wgt_in, send_sem=sw, recv_sem=rw,
        device_id={"cols": other}, device_id_type=MESH)
    swap.start()

    w = pltpu.roll(z[steps:2 * steps, :], LANES - steps, 1)
    w = jnp.where(lane < steps, w, 0.0)
    w = w + pltpu.roll(w, steps, 1) + pltpu.roll(w, 2 * steps, 1)
    w = jnp.concatenate([w, jnp.zeros((LANES - steps, LANES), jnp.float32)], axis=0)
    u = jnp.dot(spread_ref[...], w, precision=lax.Precision.HIGHEST, preferred_element_type=jnp.float32)
    high = u.astype(jnp.bfloat16).astype(jnp.float32)
    ust_ref[...] = jnp.where(lane_c < 2 * steps, high, u - high).astype(jnp.bfloat16)

    lane_p = lax.broadcasted_iota(jnp.int32, (steps, pcol), 1)
    sub_p = lax.broadcasted_iota(jnp.int32, (steps, pcol), 0)
    owner = jnp.zeros((steps, pcol), jnp.int32)
    for k in range(steps):
        owner = jnp.where(sub_p == k, site[k], owner)
    owner = owner - lane_p

    each(lambda j: second_copy(j).wait_recv())
    for c in range(cc):
        parts = [raw[g * cc + c] for g in range(rg)]
        rows = parts[0] if rg == 1 else jnp.concatenate(parts, axis=0)
        v = jnp.where(owner == c * pcol, one, 0.0) - rows
        vh = v.astype(jnp.bfloat16)
        vl = (v - vh.astype(jnp.float32)).astype(jnp.bfloat16)
        vst_ref[:, c * pcol:(c + 1) * pcol] = jnp.concatenate([vh, vl, vh], axis=0)

    swap.wait()
    total_ref[0, 0] = jnp.max(wgt[0:1, :] + wgt_in[0:1, :])
    each(lambda j: block_copy(j).wait_send())
    each(lambda j: first_copy(j).wait_send())
    each(lambda j: second_copy(j).wait_send())


def apply_kernel(k3, tile, ust_ref, vst_ref, total_ref, local, out_hbm, sum_ref, held, sems):
    copies = []
    ust = ust_ref[:, :k3]
    for i in range(local.shape[1] // tile):
        cols = slice(i * tile, (i + 1) * tile)
        held[:, cols] = local[:, cols] - jnp.dot(
            ust, vst_ref[:, cols], preferred_element_type=jnp.float32)
        copies.append(pltpu.make_async_copy(held.at[:, cols], out_hbm.at[:, cols], sems.at[i]))
        copies[-1].start()
    sum_ref[0, 0] = total_ref[0, 0]
    for copy in copies:
        copy.wait()


def on_device(n, green, sites, fields, accept):
    local = green[0]
    rows_dev, width = local.shape
    steps = sites.shape[0]
    cc = min(n, width // LANES)
    rg = n // cc
    brow = steps // (LANES // steps)
    prow, pcol = steps // rg, width // cc
    f32, i32, bf16 = jnp.float32, jnp.int32, jnp.bfloat16
    vmem = pl.BlockSpec(memory_space=pltpu.VMEM)
    smem = pl.BlockSpec(memory_space=pltpu.SMEM)
    dma = pltpu.SemaphoreType.DMA
    shape = jax.ShapeDtypeStruct
    limit = 16 * 1024 * 1024
    sizes = (n, steps, rows_dev, width, cc, rg)
    ust, vst, total = pl.pallas_call(
        functools.partial(exchange_kernel, *sizes),
        out_shape=(shape((rows_dev, LANES), bf16), shape((3 * steps, width), bf16), shape((1, 1), f32)),
        in_specs=[pl.BlockSpec(memory_space=pltpu.HBM)] * 4,
        out_specs=(vmem, vmem, smem),
        scratch_shapes=[
            pltpu.SMEM((steps,), i32),
            pltpu.VMEM((fields.shape[0] // LANES, LANES), i32),
            pltpu.SMEM((steps,), i32),
            pltpu.VMEM((rows_dev, width), f32),
            pltpu.VMEM((n, prow, pcol), f32),
            pltpu.VMEM((rows_dev, LANES), f32),
            pltpu.VMEM((n, prow, pcol), f32),
            pltpu.VMEM((prow, pcol), f32),
            pltpu.VMEM((n, prow, pcol), f32),
            pltpu.VMEM((brow, LANES), f32),
            pltpu.VMEM((n, brow, LANES), f32),
            pltpu.VMEM((8, LANES), f32),
            pltpu.VMEM((8, LANES), f32),
            dma((4,)), dma((n,)), dma((n,)), dma((n,)), dma((n,)), dma((n,)), dma((n,)), dma, dma,
        ],
        compiler_params=pltpu.CompilerParams(
            collective_id=0, has_side_effects=True, vmem_limit_bytes=54 * 1024 * 1024),
        cost_estimate=pl.CostEstimate(flops=10 ** 9, bytes_accessed=64 * 2 ** 20, transcendentals=0),
        name="exchange",
    )(sites, fields.reshape(-1, LANES), accept, local)

    tile = min(512, width)
    updated, summed = pl.pallas_call(
        functools.partial(apply_kernel, 3 * steps, tile),
        out_shape=(shape((rows_dev, width), f32), shape((1, 1), f32)),
        in_specs=[vmem, vmem, smem, vmem],
        out_specs=(pl.BlockSpec(memory_space=pltpu.HBM), smem),
        scratch_shapes=[pltpu.VMEM((rows_dev, width), f32), dma((width // tile,))],
        compiler_params=pltpu.CompilerParams(vmem_limit_bytes=limit),
        cost_estimate=pl.CostEstimate(
            flops=2 * rows_dev * width * 3 * steps, bytes_accessed=8 * rows_dev * width, transcendentals=0),
        name="apply",
    )(ust, vst, total, local)
    return updated[None], summed.reshape(())


def solution(mesh):
    in_specs = (P("cols", "rows", None), P(), P(), P())
    out_specs = (P("cols", "rows", None), P())
    return jax.shard_map(
        functools.partial(on_device, mesh.shape["rows"]),
        mesh=mesh, in_specs=in_specs, out_specs=out_specs, check_vma=False,
    )
```

```python
import functools

import jax
import jax.numpy as jnp
import numpy as np
from jax import lax
from jax.experimental import pallas as pl
from jax.experimental.pallas import tpu as pltpu
from jax.sharding import PartitionSpec as P

FLOOR = 0.25
COUPLING = 0.5
LANES = 128
MESH = pl.DeviceIdType.MESH


def exchange_kernel(n, steps, rows_dev, width, cc, rg,
                    sites_hbm, fields_hbm, accept_hbm, green_hbm,
                    vst_ref, total_ref,
                    sites_ref, fields_ref, accept_ref, local, picked, spread_ref,
                    landed, mine, raw, blk, blks, wgt, wgt_in,
                    ls, s1, r1, s2, r2, sb, rb, sw, rw):
    me = lax.axis_index("rows")
    spin = lax.axis_index("cols")
    other = 1 - spin
    prow = steps // rg
    pcol = width // cc
    per = LANES // steps
    brow = steps // per

    loads = [
        pltpu.make_async_copy(sites_hbm, sites_ref, ls.at[0]),
        pltpu.make_async_copy(accept_hbm, accept_ref, ls.at[1]),
        pltpu.make_async_copy(fields_hbm, fields_ref, ls.at[2]),
        pltpu.make_async_copy(green_hbm, local, ls.at[3]),
    ]
    for load in loads:
        load.start()

    barrier = pltpu.get_barrier_semaphore()

    def greet(j, _):
        pl.semaphore_signal(barrier, inc=1, device_id={"rows": lax.rem(me + j, n)}, device_id_type=MESH)
        return _

    lax.fori_loop(1, n, greet, 0)
    pl.semaphore_signal(barrier, inc=1, device_id={"cols": other}, device_id_type=MESH)

    first = me * rows_dev
    for load in loads:
        load.wait()
    site = [sites_ref[k] for k in range(steps)]
    lane = lax.broadcasted_iota(jnp.int32, (steps, LANES), 1)
    sub = lax.broadcasted_iota(jnp.int32, (steps, LANES), 0)
    lane_1 = lax.broadcasted_iota(jnp.int32, (1, LANES), 1)

    span = min(2 * LANES, width)
    site_sub = jnp.zeros((steps, rows_dev), jnp.int32)
    row_at = lax.broadcasted_iota(jnp.int32, (steps, rows_dev), 0)
    for k in range(steps):
        site_sub = jnp.where(row_at == k, site[k], site_sub)
    mark = lax.broadcasted_iota(jnp.int32, (steps, rows_dev), 1) + first
    chosen = jnp.where(site_sub == mark, 1.0, 0.0).astype(jnp.bfloat16)

    def split(x):
        h = x.astype(jnp.bfloat16)
        rest = x - h.astype(jnp.float32)
        m = rest.astype(jnp.bfloat16)
        return h, m, (rest - m.astype(jnp.float32)).astype(jnp.bfloat16)

    def mul(x, y):
        return jnp.dot(x, y, preferred_element_type=jnp.float32)

    for q in range(width // span):
        h, m, l = split(local[:, q * span:(q + 1) * span])
        got = mul(chosen, h) + mul(chosen, m) + mul(chosen, l)
        for t in range(span // LANES):
            p, o = divmod(q * span + t * LANES, pcol)
            for g in range(rg):
                picked[g * cc + p, :, o:o + LANES] = got[g * prow:(g + 1) * prow, t * LANES:(t + 1) * LANES]

    pl.semaphore_wait(barrier, n)

    def order(i):
        return 1 + lax.rem(i + n // 2 - 1, n - 1)

    def block_copy(j):
        to = lax.rem(me + j, n)
        return pltpu.make_async_remote_copy(
            src_ref=blk, dst_ref=blks.at[j], send_sem=sb.at[j], recv_sem=rb.at[j],
            device_id={"rows": to}, device_id_type=MESH)

    def first_copy(j):
        to = lax.rem(me + j, n)
        return pltpu.make_async_remote_copy(
            src_ref=picked.at[to], dst_ref=landed.at[j], send_sem=s1.at[j], recv_sem=r1.at[j],
            device_id={"rows": to}, device_id_type=MESH)

    def second_copy(j):
        to = lax.rem(me + j, n)
        return pltpu.make_async_remote_copy(
            src_ref=mine, dst_ref=raw.at[me], send_sem=s2.at[j], recv_sem=r2.at[j],
            device_id={"rows": to}, device_id_type=MESH)

    def each(fn):
        def body(i, _):
            fn(order(i))
            return _
        lax.fori_loop(0, n - 1, body, 0)

    each(lambda j: first_copy(j).start())

    site_lane = jnp.full((span, LANES), -1, jnp.int32)
    lane_s = lax.broadcasted_iota(jnp.int32, (span, LANES), 1)
    for k in range(steps):
        site_lane = jnp.where(lane_s == k, site[k], site_lane)
    site_lane = site_lane - lax.broadcasted_iota(jnp.int32, (span, LANES), 0)
    block = jnp.zeros((steps, LANES), jnp.float32)
    for q in range(width // span):
        wanted = jnp.where(site_lane == q * span, 1.0, 0.0).astype(jnp.bfloat16)
        pieces = []
        for t in range(span // LANES):
            p, o = divmod(q * span + t * LANES, pcol)
            parts = [picked[g * cc + p, :, o:o + LANES] for g in range(rg)]
            pieces.append(parts[0] if rg == 1 else jnp.concatenate(parts, axis=0))
        h, m, l = split(jnp.concatenate(pieces, axis=1))
        block = block + (mul(h, wanted) + mul(m, wanted) + mul(l, wanted))
    packed = []
    for q in range(brow):
        line = block[q * per:(q + 1) * per, :]
        sub_q = lax.broadcasted_iota(jnp.int32, (per, LANES), 0)
        acc = jnp.zeros((per, LANES), jnp.float32)
        for i in range(per):
            turned = line if i == 0 else pltpu.roll(line, i * steps, 1)
            acc = jnp.where(sub_q == i, turned, acc)
        packed.append(jnp.sum(acc, axis=0, keepdims=True))
    blk[...] = jnp.concatenate(packed, axis=0)
    each(lambda j: block_copy(j).start())

    spread = jnp.zeros((rows_dev, LANES), jnp.float32)
    lane_c = lax.broadcasted_iota(jnp.int32, (rows_dev, LANES), 1)
    for q in range(width // span):
        wanted = jnp.where(site_lane == q * span, 1.0, 0.0).astype(jnp.bfloat16)
        h, m, l = split(local[:, q * span:(q + 1) * span])
        spread = spread + (mul(h, wanted) + mul(m, wanted) + mul(l, wanted))
    spread_ref[...] = spread

    each(lambda j: first_copy(j).wait_recv())
    chunk = picked[me]
    for j in range(1, n):
        chunk = chunk + landed[j]
    mine[...] = chunk
    raw[me] = chunk
    each(lambda j: second_copy(j).start())

    each(lambda j: block_copy(j).wait_recv())
    packed = blk[...]
    for j in range(1, n):
        packed = packed + blks[j]
    block = jnp.zeros((steps, LANES), jnp.float32)
    for k in range(steps):
        line = jnp.broadcast_to(packed[k // per:k // per + 1, :], (8, LANES))
        back = (LANES - (k % per) * steps) % LANES
        if back:
            line = pltpu.roll(line, back, 1)
        block = jnp.where(sub == k, jnp.broadcast_to(line[0:1, :], (steps, LANES)), block)
    one = jnp.float32(1.0)
    block = jnp.where(lane < steps, block, jnp.where(lane == sub + steps, one, 0.0))
    under = jnp.where(lane == sub, one, 0.0)
    z = jnp.concatenate([block, under], axis=0)
    same = np.float32(np.exp(np.float32(-2.0 * COUPLING))) - np.float32(1.0)
    differ = np.float32(np.exp(np.float32(2.0 * COUPLING))) - np.float32(1.0)
    fields = fields_ref[...]
    place = (lax.broadcasted_iota(jnp.int32, fields.shape, 0) * LANES
             + lax.broadcasted_iota(jnp.int32, fields.shape, 1))
    deltas = []
    for k in range(steps):
        found = jnp.where(place == site[k], fields.astype(jnp.float32), 0.0)
        found = jnp.sum(jnp.sum(found, axis=0, keepdims=True), axis=1, keepdims=True)
        found = jnp.broadcast_to(found, (1, LANES)) * jnp.ones((1, LANES), jnp.float32)
        kind = jnp.where(spin + 0 * lane_1 == 0, found, 1.0 - found)
        deltas.append(same + kind * (differ - same))
    ratios = jnp.ones((1, LANES), jnp.float32)
    flags = jnp.zeros((1, LANES), jnp.float32)
    for k in range(steps):
        flag = accept_ref[k].astype(jnp.float32)
        delta = deltas[k]
        row = z[k:k + 1, :]
        column = jnp.broadcast_to(z[:, k:k + 1], z.shape)
        diag = column[k:k + 1, :]
        ratio = jnp.maximum(1.0 + delta * (1.0 - diag), FLOOR)
        coef = (flag * delta) / ratio
        fresh = jnp.where(lane_1 == k, one, 0.0) - row
        z = z - column * (coef * fresh)
        ratios = jnp.where(lane_1 == k, ratio, ratios)
        flags = jnp.where(lane_1 == k, flag, flags)
    weight = jnp.sum(flags * jnp.log(ratios), axis=1, keepdims=True)
    wgt[...] = jnp.broadcast_to(weight, (8, LANES))
    swap = pltpu.make_async_remote_copy(
        src_ref=wgt, dst_ref=wgt_in, send_sem=sw, recv_sem=rw,
        device_id={"cols": other}, device_id_type=MESH)
    swap.start()

    w = pltpu.roll(z[steps:2 * steps, :], LANES - steps, 1)
    w = jnp.where(lane < steps, w, 0.0)
    w = w + pltpu.roll(w, steps, 1) + pltpu.roll(w, 2 * steps, 1)
    w = jnp.concatenate([w, jnp.zeros((LANES - steps, LANES), jnp.float32)], axis=0)
    u = jnp.dot(spread_ref[...], w, precision=lax.Precision.HIGHEST, preferred_element_type=jnp.float32)
    high = u.astype(jnp.bfloat16).astype(jnp.float32)
    left = jnp.where(lane_c < 2 * steps, high, u - high).astype(jnp.bfloat16)
    for g in range(-(-rows_dev // (3 * steps))):
        part = left[g * 3 * steps:(g + 1) * 3 * steps, :]
        vst_ref[:part.shape[0], width + g * LANES:width + (g + 1) * LANES] = part

    lane_p = lax.broadcasted_iota(jnp.int32, (steps, pcol), 1)
    sub_p = lax.broadcasted_iota(jnp.int32, (steps, pcol), 0)
    owner = jnp.zeros((steps, pcol), jnp.int32)
    for k in range(steps):
        owner = jnp.where(sub_p == k, site[k], owner)
    owner = owner - lane_p

    each(lambda j: second_copy(j).wait_recv())
    for c in range(cc):
        parts = [raw[g * cc + c] for g in range(rg)]
        rows = parts[0] if rg == 1 else jnp.concatenate(parts, axis=0)
        v = jnp.where(owner == c * pcol, one, 0.0) - rows
        vh = v.astype(jnp.bfloat16)
        vl = (v - vh.astype(jnp.float32)).astype(jnp.bfloat16)
        vst_ref[:, c * pcol:(c + 1) * pcol] = jnp.concatenate([vh, vl, vh], axis=0)

    swap.wait()
    total_ref[0, 0] = jnp.max(wgt[0:1, :] + wgt_in[0:1, :])
    each(lambda j: block_copy(j).wait_send())
    each(lambda j: first_copy(j).wait_send())
    each(lambda j: second_copy(j).wait_send())


def apply_kernel(k3, tile, vst_ref, total_ref, local, out_hbm, sum_ref, held, sems):
    copies = []
    rows_dev, width = local.shape
    groups = [vst_ref[:min(k3, rows_dev - g * k3), width + g * LANES:width + (g + 1) * LANES]
              for g in range(-(-rows_dev // k3))]
    ust = (groups[0] if len(groups) == 1 else jnp.concatenate(groups, axis=0))[:, :k3]
    for i in range(local.shape[1] // tile):
        cols = slice(i * tile, (i + 1) * tile)
        held[:, cols] = local[:, cols] - jnp.dot(
            ust, vst_ref[:, cols], preferred_element_type=jnp.float32)
        copies.append(pltpu.make_async_copy(held.at[:, cols], out_hbm.at[:, cols], sems.at[i]))
        copies[-1].start()
    sum_ref[0, 0] = total_ref[0, 0]
    for copy in copies:
        copy.wait()


def on_device(n, green, sites, fields, accept):
    local = green[0]
    rows_dev, width = local.shape
    steps = sites.shape[0]
    cc = min(n, width // LANES)
    rg = n // cc
    brow = steps // (LANES // steps)
    prow, pcol = steps // rg, width // cc
    f32, i32, bf16 = jnp.float32, jnp.int32, jnp.bfloat16
    vmem = pl.BlockSpec(memory_space=pltpu.VMEM)
    smem = pl.BlockSpec(memory_space=pltpu.SMEM)
    dma = pltpu.SemaphoreType.DMA
    shape = jax.ShapeDtypeStruct
    limit = 16 * 1024 * 1024
    sizes = (n, steps, rows_dev, width, cc, rg)
    groups = -(-rows_dev // (3 * steps))
    vst, total = pl.pallas_call(
        functools.partial(exchange_kernel, *sizes),
        out_shape=(shape((3 * steps, width + groups * LANES), bf16), shape((1, 1), f32)),
        in_specs=[pl.BlockSpec(memory_space=pltpu.HBM)] * 4,
        out_specs=(vmem, smem),
        scratch_shapes=[
            pltpu.SMEM((steps,), i32),
            pltpu.VMEM((fields.shape[0] // LANES, LANES), i32),
            pltpu.SMEM((steps,), i32),
            pltpu.VMEM((rows_dev, width), f32),
            pltpu.VMEM((n, prow, pcol), f32),
            pltpu.VMEM((rows_dev, LANES), f32),
            pltpu.VMEM((n, prow, pcol), f32),
            pltpu.VMEM((prow, pcol), f32),
            pltpu.VMEM((n, prow, pcol), f32),
            pltpu.VMEM((brow, LANES), f32),
            pltpu.VMEM((n, brow, LANES), f32),
            pltpu.VMEM((8, LANES), f32),
            pltpu.VMEM((8, LANES), f32),
            dma((4,)), dma((n,)), dma((n,)), dma((n,)), dma((n,)), dma((n,)), dma((n,)), dma, dma,
        ],
        compiler_params=pltpu.CompilerParams(
            collective_id=0, has_side_effects=True, vmem_limit_bytes=54 * 1024 * 1024),
        cost_estimate=pl.CostEstimate(flops=10 ** 9, bytes_accessed=64 * 2 ** 20, transcendentals=0),
        name="exchange",
    )(sites, fields.reshape(-1, LANES), accept, local)

    tile = min(512, width)
    updated, summed = pl.pallas_call(
        functools.partial(apply_kernel, 3 * steps, tile),
        out_shape=(shape((rows_dev, width), f32), shape((1, 1), f32)),
        in_specs=[vmem, smem, vmem],
        out_specs=(pl.BlockSpec(memory_space=pltpu.HBM), smem),
        scratch_shapes=[pltpu.VMEM((rows_dev, width), f32), dma((width // tile,))],
        compiler_params=pltpu.CompilerParams(vmem_limit_bytes=limit),
        cost_estimate=pl.CostEstimate(
            flops=2 * rows_dev * width * 3 * steps, bytes_accessed=8 * rows_dev * width, transcendentals=0),
        name="apply",
    )(vst, total, local)
    return updated[None], summed.reshape(())


def solution(mesh):
    in_specs = (P("cols", "rows", None), P(), P(), P())
    out_specs = (P("cols", "rows", None), P())
    return jax.shard_map(
        functools.partial(on_device, mesh.shape["rows"]),
        mesh=mesh, in_specs=in_specs, out_specs=out_specs, check_vma=False,
    )
```
